32 devices in a mesh: shots: 1, gx: 32 (over z, y, x, core), gy: 1.
Axes of the slice: x: 2, y: 2, z: 4, core: 2. Of those that a mesh axis runs over, the one named last changes fastest.
Arguments:
- pressure: float32 [128, 256, 128], P(None, ('shots', 'gx'), 'gy'), may hold values from -6 to 6
- pressure_prior: float32 [128, 256, 128], P(None, ('shots', 'gx'), 'gy'), may hold values from -6 to 6
- courant_square: bfloat16 [128, 256, 128], P(None, 'gx', 'gy'), may hold values from 0.049804688 to 0.1796875
- wavelet: float32 [16], P('shots'), may hold values from -4 to 4
- delay_steps: int32 [256, 128], P(('shots', 'gx'), 'gy'), may hold values from 0 to 7
- source_depth: int32 [256, 128], P(('shots', 'gx'), 'gy'), may hold values from 4 to 31
- receiver_depth: int32 [256, 128], P(('shots', 'gx'), 'gy'), may hold values from 0 to 31
- receiver_field: float32 [128, 256, 128], P(None, ('shots', 'gx'), 'gy'), may hold values from -6 to 6
Outputs:
- pressure_final: float32 [128, 256, 128], P(None, ('shots', 'gx'), 'gy')
- image: float32 [128, 256, 128], P('gx', 'shots', 'gy')
The draws below stay inside these ranges and needn't reach their ends.
All inputs are finite; a program needn't handle non-finite values.
Results may differ from the reference program's by a relative error of at most 0.00035.
Values sent between devices are 32-bit elements; how exact they have to be, the bound alone decides.
A program may use at most 64 MiB of HBM per device.

```python
import math
import jax
import jax.numpy as jnp

STEPS = 8
DMAX = 8
WAVE = 16
NX = 256
NY = 128
NZ = 128


def plant(array, stream_key, low, top_value):
    shape = array.shape
    spot = [jax.random.randint(jax.random.fold_in(stream_key, axis), (), 0, shape[axis]) for axis in range(len(shape))]
    array = array.at[tuple(spot)].set(low)
    longest = shape.index(max(shape))
    spot[longest] = (spot[longest] + 1) % shape[longest]
    return array.at[tuple(spot)].set(top_value)


def block_levels(rng, dims, cuts, low, high):
    def one(axis_at, parts):
        steps = jax.random.uniform(jax.random.fold_in(jax.random.fold_in(rng, 6), axis_at), (parts,), jnp.float32, low / len(cuts), high / len(cuts))
        return jnp.repeat(jnp.exp(steps), dims[axis_at] // parts).reshape((-1,) + (1,) * (len(dims) - axis_at - 1))

    factor_of = one(*cuts[0])
    for cut in cuts[1:]:
        factor_of = factor_of * one(*cut)
    return factor_of


def gaussian(key, dims, scale, most, split=(), kind=jnp.bfloat16):
    gain = block_levels(key, dims, split, -0.22, 0.18) if split else 1.0
    entries = jax.random.normal(key, dims, jnp.float32) * scale * gain
    return jnp.minimum(jnp.maximum(entries, -most), most).astype(kind)


def setup_inputs(seed: int = 0, part: int = 0) -> dict:
    seeds = jax.random.split(jax.random.key(seed), 9)
    own_keys = jax.random.split(jax.random.fold_in(seeds[8], part), 9)
    pressure = gaussian(own_keys[0], (NZ, NX, NY), 1.0, 6.0, ((1, 32),), jnp.float32)
    pressure_prior = gaussian(own_keys[1], (NZ, NX, NY), 1.0, 6.0, ((1, 32),), jnp.float32)
    courant_square = jnp.clip(jnp.exp(math.log(0.1796875) - 1.2831101 * jax.random.uniform(seeds[2], (NZ, NX, NY), jnp.float32) ** block_levels(seeds[2], (NZ, NX, NY), ((1, 32),), -0.2, 0.2)), 0.049804688, 0.1796875).astype(jnp.bfloat16)
    wavelet = gaussian(own_keys[3], (WAVE,), 1.0, 4.0, (), jnp.float32)
    delay_steps = plant(jax.random.randint(own_keys[4], (NX, NY), 0, DMAX), jax.random.fold_in(own_keys[4], 1), 0, DMAX - 1).astype(jnp.int32)
    source_depth = plant(jax.random.randint(own_keys[5], (NX, NY), 4, 32), jax.random.fold_in(own_keys[5], 1), 4, 31).astype(jnp.int32)
    receiver_depth = plant(jax.random.randint(own_keys[6], (NX, NY), 0, NZ // 4), jax.random.fold_in(own_keys[6], 1), 0, (NZ // 4) - 1).astype(jnp.int32)
    receiver_field = gaussian(own_keys[7], (NZ, NX, NY), 1.0, 6.0, ((1, 32),), jnp.float32)
    return dict(pressure=pressure, pressure_prior=pressure_prior, courant_square=courant_square, wavelet=wavelet, delay_steps=delay_steps, source_depth=source_depth, receiver_depth=receiver_depth, receiver_field=receiver_field)


CENTER = -205.0 / 72.0
COEFS = (1.6, -0.2, 8.0 / 315.0, -1.0 / 560.0)


def laplacian(field):
    depth, width, length = field.shape
    padded = jnp.pad(field, 4)
    total = (3.0 * CENTER) * field
    for k in range(1, 5):
        near = padded[4 + k:4 + k + depth, 4:4 + width, 4:4 + length] + padded[4 - k:4 - k + depth, 4:4 + width, 4:4 + length]
        near = near + padded[4:4 + depth, 4 + k:4 + k + width, 4:4 + length] + padded[4:4 + depth, 4 - k:4 - k + width, 4:4 + length]
        near = near + padded[4:4 + depth, 4:4 + width, 4 + k:4 + k + length] + padded[4:4 + depth, 4:4 + width, 4 - k:4 - k + length]
        total = total + COEFS[k - 1] * near
    return total


def injection(step, wavelet, delay_steps, source_depth, depth):
    picks = jnp.arange(wavelet.shape[0], dtype=jnp.int32)
    onehot = (picks[:, None, None] == (delay_steps + step)[None]).astype(wavelet.dtype)
    amplitude = jnp.sum(onehot * wavelet[:, None, None], axis=0)
    levels = jnp.arange(depth, dtype=jnp.int32)[:, None, None]
    return jnp.where(levels == source_depth[None], amplitude[None], jnp.zeros_like(amplitude)[None])


def reference(pressure, pressure_prior, courant_square, wavelet, delay_steps, source_depth, receiver_depth, receiver_field):
    depth = pressure.shape[0]
    coefficient = courant_square.astype(jnp.float32)
    current, prior = pressure, pressure_prior
    for step in range(STEPS):
        nxt = 2.0 * current - prior + coefficient * laplacian(current) + injection(step, wavelet, delay_steps, source_depth, depth)
        prior, current = current, nxt
    levels = jnp.arange(depth, dtype=jnp.int32)[:, None, None]
    masked = jnp.where(levels >= receiver_depth[None], receiver_field, jnp.zeros_like(receiver_field))
    product = current * masked
    padded = jnp.pad(product, ((1, 1), (0, 0), (0, 0)))
    image = 2.0 * product - padded[:-2] - padded[2:]
    return current, image
```

```python
import functools

import jax
import jax.numpy as jnp
from jax import lax
from jax.experimental import pallas as pl
from jax.experimental.pallas import tpu as pltpu
from jax.sharding import PartitionSpec as P

STEPS = 8
REACH = 4
CENTER = -205.0 / 72.0
COEFS = (1.6, -0.2, 8.0 / 315.0, -1.0 / 560.0)
CHUNKS = 4
GROUP = 8


def kernel(
    nx,
    ny,
    pressure,
    prior,
    courant,
    wavelet,
    delay,
    sdepth,
    rdepth,
    receiver,
    final,
    image,
    field,
    side,
    prior_v,
    courant_v,
    receiver_v,
    amp,
    product,
    slab,
    local_sem,
    send_sem,
    recv_sem,
    side_send,
    side_recv,
    out_sem,
    img_send,
    img_recv,
):
    depth, width, length = pressure.shape
    rows = depth // CHUNKS
    slab_depth = depth // nx
    me = lax.axis_index("gx")
    mine = lax.axis_index("gy")

    local = [
        pltpu.make_async_copy(
            pressure, field.at[0, pl.ds(REACH, depth), pl.ds(REACH, width), :], local_sem.at[0]
        ),
        pltpu.make_async_copy(prior, prior_v, local_sem.at[1]),
        pltpu.make_async_copy(courant, courant_v, local_sem.at[2]),
        pltpu.make_async_copy(receiver, receiver_v, local_sem.at[3]),
    ]
    for copy in local:
        copy.start()

    barrier = pltpu.get_barrier_semaphore()
    for j in range(1, nx):
        pl.semaphore_signal(
            barrier,
            inc=1,
            device_id={"gx": lax.rem(me + j, nx)},
            device_id_type=pl.DeviceIdType.MESH,
        )
    for j in range(1, ny):
        pl.semaphore_signal(
            barrier,
            inc=1,
            device_id={"gy": lax.rem(mine + j, ny)},
            device_id_type=pl.DeviceIdType.MESH,
        )

    rim = jnp.zeros((REACH, width + 2 * REACH, length), jnp.float32)
    for t in range(STEPS):
        field[t, pl.ds(0, REACH), :, :] = rim
        field[t, pl.ds(REACH + depth, REACH), :, :] = rim

    def clear(at):
        def one(i, carry):
            t = i // CHUNKS
            c = i % CHUNKS
            field[t, pl.ds(REACH + c * rows, rows), pl.ds(at, REACH), :] = jnp.zeros(
                (rows, REACH, length), jnp.float32
            )
            return carry

        lax.fori_loop(0, STEPS * CHUNKS, one, 0)

    @pl.when(me == 0)
    def _():
        clear(0)

    @pl.when(me == nx - 1)
    def _():
        clear(REACH + width)

    if ny > 1:

        def clear_side(k):
            def one(i, carry):
                t = i // CHUNKS
                c = i % CHUNKS
                side[t, k, pl.ds(c * rows, rows), :, :] = jnp.zeros(
                    (rows, width, length), jnp.float32
                )
                return carry

            lax.fori_loop(0, STEPS * CHUNKS, one, 0)

        @pl.when(mine == 0)
        def _():
            clear_side(0)

        @pl.when(mine == ny - 1)
        def _():
            clear_side(1)

    late = delay[...]
    for t in range(STEPS):
        total = jnp.zeros((width, length), jnp.float32)
        for pick in range(wavelet.shape[0]):
            total = total + jnp.where(late + t == pick, wavelet[pick], 0.0)
        amp[t] = total

    if nx + ny > 2:
        pl.semaphore_wait(barrier, nx + ny - 2)

    def span(c):
        return pl.ds(REACH + c * rows, rows)

    def face(t, c, way):
        source = REACH + width - REACH if way == 0 else REACH
        target = 0 if way == 0 else REACH + width
        peer = lax.rem(me + 1, nx) if way == 0 else lax.rem(me + nx - 1, nx)
        return pltpu.make_async_remote_copy(
            src_ref=field.at[t, span(c), pl.ds(source, REACH), :],
            dst_ref=field.at[t, span(c), pl.ds(target, REACH), :],
            send_sem=send_sem.at[t, c, way],
            recv_sem=recv_sem.at[t, c, way],
            device_id={"gx": peer},
            device_id_type=pl.DeviceIdType.MESH,
        )

    def flank(t, c, way):
        peer = lax.rem(mine + 1, ny) if way == 0 else lax.rem(mine + ny - 1, ny)
        return pltpu.make_async_remote_copy(
            src_ref=field.at[t, span(c), pl.ds(REACH, width), :],
            dst_ref=side.at[t, way, pl.ds(c * rows, rows), :, :],
            send_sem=side_send.at[t, c, way],
            recv_sem=side_recv.at[t, c, way],
            device_id={"gy": peer},
            device_id_type=pl.DeviceIdType.MESH,
        )

    def each_face(t, c, act, sending):
        lower, upper = (me > 0, me < nx - 1)
        if nx > 1:
            for way in (0, 1):
                there = upper if (way == 0) == sending else lower

                @pl.when(there)
                def _():
                    act(face(t, c, way))

        if ny > 1:
            for way in (0, 1):
                there = mine < ny - 1 if (way == 0) == sending else mine > 0

                @pl.when(there)
                def _():
                    act(flank(t, c, way))

    def send(t, c):
        each_face(t, c, lambda copy: copy.start(), True)

    def sent(t, c):
        each_face(t, c, lambda copy: copy.wait_send(), True)

    def arrived(t, c):
        each_face(t, c, lambda copy: copy.wait_recv(), False)

    local[0].wait()
    for c in range(CHUNKS):
        send(0, c)
    local[1].wait()
    local[2].wait()

    lanes = lax.broadcasted_iota(jnp.int32, (width, length), 1)
    ahead = [jnp.where(lanes < length - k, COEFS[k - 1], 0.0) for k in range(1, REACH + 1)]
    behind = [jnp.where(lanes >= k, COEFS[k - 1], 0.0) for k in range(1, REACH + 1)]
    origin = sdepth[...]

    def advance(t, z, old):
        own = pl.ds(REACH, width)
        v = field[t, pl.ds(REACH + z, GROUP), own, :]
        total = (3.0 * CENTER) * v
        for k in range(1, REACH + 1):
            near = (
                field[t, pl.ds(REACH + z + k, GROUP), own, :]
                + field[t, pl.ds(REACH + z - k, GROUP), own, :]
            )
            near = near + (
                field[t, pl.ds(REACH + z, GROUP), pl.ds(REACH + k, width), :]
                + field[t, pl.ds(REACH + z, GROUP), pl.ds(REACH - k, width), :]
            )
            total = total + COEFS[k - 1] * near
            up = pltpu.roll(v, length - k, 2)
            down = pltpu.roll(v, k, 2)
            if ny > 1:
                low = pltpu.roll(side[t, 0, pl.ds(z, GROUP), :, :], k, 2)
                high = pltpu.roll(side[t, 1, pl.ds(z, GROUP), :, :], length - k, 2)
                up = jnp.where((lanes < length - k)[None], up, high)
                down = jnp.where((lanes >= k)[None], down, low)
                total = total + COEFS[k - 1] * (up + down)
            else:
                total = total + ahead[k - 1][None] * up + behind[k - 1][None] * down
        strength = courant_v[pl.ds(z, GROUP), :, :].astype(jnp.float32)
        levels = lax.broadcasted_iota(jnp.int32, (GROUP, width, length), 0) + z
        shot = jnp.where(levels == origin[None], amp[t][None], 0.0)
        return 2.0 * v - old + strength * total + shot

    def first_chunk(c, carry):
        arrived(0, c)

        def group(g, inner):
            z = c * rows + g * GROUP
            new = advance(0, z, prior_v[pl.ds(z, GROUP), :, :])
            field[1, pl.ds(REACH + z, GROUP), pl.ds(REACH, width), :] = new
            return inner

        lax.fori_loop(0, rows // GROUP, group, 0)
        send(1, c)
        return carry

    lax.fori_loop(0, CHUNKS, first_chunk, 0)

    def step(i, carry):
        t = i // CHUNKS
        c = i % CHUNKS
        arrived(t, c)

        def group(g, inner):
            z = c * rows + g * GROUP
            old = field[t - 1, pl.ds(REACH + z, GROUP), pl.ds(REACH, width), :]
            new = advance(t, z, old)
            field[t + 1, pl.ds(REACH + z, GROUP), pl.ds(REACH, width), :] = new
            return inner

        lax.fori_loop(0, rows // GROUP, group, 0)

        @pl.when(t < STEPS - 1)
        def _():
            send(t + 1, c)

        return carry

    lax.fori_loop(CHUNKS, STEPS * CHUNKS, step, 0)

    done = pltpu.make_async_copy(
        field.at[STEPS, pl.ds(REACH, depth), pl.ds(REACH, width), :], final, out_sem.at[0]
    )
    done.start()

    local[3].wait()
    ground = rdepth[...]
    product[pl.ds(0, 1), :, :] = jnp.zeros((1, width, length), jnp.float32)
    product[pl.ds(depth + 1, 1), :, :] = jnp.zeros((1, width, length), jnp.float32)

    def multiply(g, carry):
        z = g * GROUP
        levels = lax.broadcasted_iota(jnp.int32, (GROUP, width, length), 0) + z
        masked = jnp.where(levels >= ground[None], receiver_v[pl.ds(z, GROUP), :, :], 0.0)
        product[pl.ds(1 + z, GROUP), :, :] = (
            field[STEPS, pl.ds(REACH + z, GROUP), pl.ds(REACH, width), :] * masked
        )
        return carry

    lax.fori_loop(0, depth // GROUP, multiply, 0)

    def landing(who):
        return image.at[:, pl.ds(pl.multiple_of(who * width, width), width), :]

    def piece(peer):
        return pltpu.make_async_remote_copy(
            src_ref=slab.at[pl.ds(peer * slab_depth, slab_depth), :, :],
            dst_ref=landing(me),
            send_sem=img_send.at[peer],
            recv_sem=img_recv.at[me],
            device_id={"gx": peer},
            device_id_type=pl.DeviceIdType.MESH,
        )

    def kept():
        return pltpu.make_async_copy(
            slab.at[pl.ds(me * slab_depth, slab_depth), :, :], landing(me), out_sem.at[1]
        )

    def filtered(peer):
        z = peer * slab_depth
        slab[pl.ds(z, slab_depth), :, :] = (
            2.0 * product[pl.ds(1 + z, slab_depth), :, :]
            - product[pl.ds(z, slab_depth), :, :]
            - product[pl.ds(2 + z, slab_depth), :, :]
        )

    def ship(j, carry):
        peer = lax.rem(me + j, nx)
        filtered(peer)
        piece(peer).start()
        return carry

    lax.fori_loop(1, nx, ship, 0)
    filtered(me)
    kept().start()

    def drain(i, carry):
        sent(i // CHUNKS, i % CHUNKS)
        return carry

    lax.fori_loop(0, STEPS * CHUNKS, drain, 0)

    def finish(j, carry):
        peer = lax.rem(me + j, nx)
        piece(peer).wait_send()
        came = lax.rem(me + nx - j, nx)
        pltpu.make_async_remote_copy(
            src_ref=slab.at[pl.ds(me * slab_depth, slab_depth), :, :],
            dst_ref=landing(came),
            send_sem=img_send.at[came],
            recv_sem=img_recv.at[came],
            device_id={"gx": came},
            device_id_type=pl.DeviceIdType.MESH,
        ).wait_recv()
        return carry

    lax.fori_loop(1, nx, finish, 0)
    kept().wait()
    done.wait()


def solution(mesh):
    nx, ny = mesh.shape["gx"], mesh.shape["gy"]

    def shards(
        pressure, prior, courant, wavelet, delay, sdepth, rdepth, receiver
    ):
        depth, width, length = pressure.shape
        hbm = pl.BlockSpec(memory_space=pl.ANY)
        vmem = pl.BlockSpec(memory_space=pltpu.VMEM)
        smem = pl.BlockSpec(memory_space=pltpu.SMEM)
        flat = (depth, width, length)
        sides = (STEPS, 2, depth, width, length) if ny > 1 else (1, 1, 1, width, length)
        return pl.pallas_call(
            functools.partial(kernel, nx, ny),
            out_shape=(
                jax.ShapeDtypeStruct(flat, jnp.float32),
                jax.ShapeDtypeStruct((depth // nx, width * nx, length), jnp.float32),
            ),
            in_specs=[hbm, hbm, hbm, smem, vmem, vmem, vmem, hbm],
            out_specs=(hbm, hbm),
            scratch_shapes=[
                pltpu.VMEM((STEPS + 1, depth + 2 * REACH, width + 2 * REACH, length), jnp.float32),
                pltpu.VMEM(sides, jnp.float32),
                pltpu.VMEM(flat, jnp.float32),
                pltpu.VMEM(flat, jnp.bfloat16),
                pltpu.VMEM(flat, jnp.float32),
                pltpu.VMEM((STEPS, width, length), jnp.float32),
                pltpu.VMEM((depth + 2, width, length), jnp.float32),
                pltpu.VMEM(flat, jnp.float32),
                pltpu.SemaphoreType.DMA((4,)),
                pltpu.SemaphoreType.DMA((STEPS, CHUNKS, 2)),
                pltpu.SemaphoreType.DMA((STEPS, CHUNKS, 2)),
                pltpu.SemaphoreType.DMA((STEPS, CHUNKS, 2)),
                pltpu.SemaphoreType.DMA((STEPS, CHUNKS, 2)),
                pltpu.SemaphoreType.DMA((2,)),
                pltpu.SemaphoreType.DMA((nx,)),
                pltpu.SemaphoreType.DMA((nx,)),
            ],
            compiler_params=pltpu.CompilerParams(
                collective_id=0, has_side_effects=True, vmem_limit_bytes=48 * 1024 * 1024
            ),
        )(pressure, prior, courant, wavelet, delay, sdepth, rdepth, receiver)

    in_specs = (
        P(None, ("shots", "gx"), "gy"),
        P(None, ("shots", "gx"), "gy"),
        P(None, "gx", "gy"),
        P("shots"),
        P(("shots", "gx"), "gy"),
        P(("shots", "gx"), "gy"),
        P(("shots", "gx"), "gy"),
        P(None, ("shots", "gx"), "gy"),
    )
    out_specs = (P(None, ("shots", "gx"), "gy"), P("gx", "shots", "gy"))
    return jax.shard_map(shards, mesh=mesh, in_specs=in_specs, out_specs=out_specs, check_vma=False)
```

```python
import functools

import jax
import jax.numpy as jnp
from jax import lax
from jax.experimental import pallas as pl
from jax.experimental.pallas import tpu as pltpu
from jax.sharding import PartitionSpec as P

STEPS = 8
REACH = 4
CENTER = -205.0 / 72.0
COEFS = (1.6, -0.2, 8.0 / 315.0, -1.0 / 560.0)
CHUNKS = 4
GROUP = 8


def kernel(
    nx,
    ny,
    pressure,
    prior,
    courant,
    wavelet,
    delay,
    sdepth,
    rdepth,
    receiver,
    final,
    image,
    field,
    side,
    prior_v,
    courant_v,
    receiver_v,
    amp,
    product,
    slab,
    weights,
    wave_v,
    delay_v,
    sdepth_v,
    rdepth_v,
    local_sem,
    send_sem,
    recv_sem,
    side_send,
    side_recv,
    out_sem,
    img_send,
    img_recv,
):
    depth, width, length = pressure.shape
    rows = depth // CHUNKS
    slab_depth = depth // nx
    me = lax.axis_index("gx")
    mine = lax.axis_index("gy")

    local = [
        pltpu.make_async_copy(
            pressure, field.at[0, pl.ds(REACH, depth), pl.ds(REACH, width), :], local_sem.at[0]
        ),
        pltpu.make_async_copy(prior, prior_v, local_sem.at[1]),
        pltpu.make_async_copy(courant, courant_v, local_sem.at[2]),
        pltpu.make_async_copy(receiver, receiver_v, local_sem.at[3]),
        pltpu.make_async_copy(wavelet, wave_v, local_sem.at[4]),
        pltpu.make_async_copy(delay, delay_v, local_sem.at[5]),
        pltpu.make_async_copy(sdepth, sdepth_v, local_sem.at[6]),
        pltpu.make_async_copy(rdepth, rdepth_v, local_sem.at[7]),
    ]
    for copy in local:
        copy.start()

    barrier = pltpu.get_barrier_semaphore()
    for j in range(1, nx):
        pl.semaphore_signal(
            barrier,
            inc=1,
            device_id={"gx": lax.rem(me + j, nx)},
            device_id_type=pl.DeviceIdType.MESH,
        )
    for j in range(1, ny):
        pl.semaphore_signal(
            barrier,
            inc=1,
            device_id={"gy": lax.rem(mine + j, ny)},
            device_id_type=pl.DeviceIdType.MESH,
        )

    rim = jnp.zeros((REACH, width + 2 * REACH, length), jnp.float32)
    for t in range(STEPS):
        field[t, pl.ds(0, REACH), :, :] = rim
        field[t, pl.ds(REACH + depth, REACH), :, :] = rim

    def clear(at):
        def one(i, carry):
            t = i // CHUNKS
            c = i % CHUNKS
            field[t, pl.ds(REACH + c * rows, rows), pl.ds(at, REACH), :] = jnp.zeros(
                (rows, REACH, length), jnp.float32
            )
            return carry

        lax.fori_loop(0, STEPS * CHUNKS, one, 0)

    @pl.when(me == 0)
    def _():
        clear(0)

    @pl.when(me == nx - 1)
    def _():
        clear(REACH + width)

    if ny > 1:

        def clear_side(k):
            def one(i, carry):
                t = i // CHUNKS
                c = i % CHUNKS
                side[t, k, pl.ds(c * rows, rows), :, :] = jnp.zeros(
                    (rows, width, length), jnp.float32
                )
                return carry

            lax.fori_loop(0, STEPS * CHUNKS, one, 0)

        @pl.when(mine == 0)
        def _():
            clear_side(0)

        @pl.when(mine == ny - 1)
        def _():
            clear_side(1)

    local[4].wait()
    local[5].wait()
    late = delay_v[...]
    for t in range(STEPS):
        total = jnp.zeros((width, length), jnp.float32)
        for pick in range(wavelet.shape[0]):
            total = total + jnp.where(late + t == pick, wave_v[pick], 0.0)
        amp[t] = total

    if nx + ny > 2:
        pl.semaphore_wait(barrier, nx + ny - 2)

    def span(c):
        return pl.ds(REACH + c * rows, rows)

    def face(t, c, way):
        source = REACH + width - REACH if way == 0 else REACH
        target = 0 if way == 0 else REACH + width
        peer = lax.rem(me + 1, nx) if way == 0 else lax.rem(me + nx - 1, nx)
        return pltpu.make_async_remote_copy(
            src_ref=field.at[t, span(c), pl.ds(source, REACH), :],
            dst_ref=field.at[t, span(c), pl.ds(target, REACH), :],
            send_sem=send_sem.at[t, c, way],
            recv_sem=recv_sem.at[t, c, way],
            device_id={"gx": peer},
            device_id_type=pl.DeviceIdType.MESH,
        )

    def flank(t, c, way):
        peer = lax.rem(mine + 1, ny) if way == 0 else lax.rem(mine + ny - 1, ny)
        return pltpu.make_async_remote_copy(
            src_ref=field.at[t, span(c), pl.ds(REACH, width), :],
            dst_ref=side.at[t, way, pl.ds(c * rows, rows), :, :],
            send_sem=side_send.at[t, c, way],
            recv_sem=side_recv.at[t, c, way],
            device_id={"gy": peer},
            device_id_type=pl.DeviceIdType.MESH,
        )

    def each_face(t, c, act, sending):
        lower, upper = (me > 0, me < nx - 1)
        if nx > 1:
            for way in (0, 1):
                there = upper if (way == 0) == sending else lower

                @pl.when(there)
                def _():
                    act(face(t, c, way))

        if ny > 1:
            for way in (0, 1):
                there = mine < ny - 1 if (way == 0) == sending else mine > 0

                @pl.when(there)
                def _():
                    act(flank(t, c, way))

    def send(t, c):
        each_face(t, c, lambda copy: copy.start(), True)

    def sent(t, c):
        each_face(t, c, lambda copy: copy.wait_send(), True)

    def arrived(t, c):
        each_face(t, c, lambda copy: copy.wait_recv(), False)

    local[0].wait()
    for c in range(CHUNKS):
        send(0, c)
    local[1].wait()
    local[2].wait()

    lanes = lax.broadcasted_iota(jnp.int32, (width, length), 1)
    start = lax.broadcasted_iota(jnp.int32, (length, length), 0)
    gap = jnp.abs(start - lax.broadcasted_iota(jnp.int32, (length, length), 1))
    band = jnp.where(gap == 0, 3.0 * CENTER, 0.0)
    for k in range(1, REACH + 1):
        band = jnp.where(gap == k, COEFS[k - 1], band)
    band_high = band.astype(jnp.bfloat16)
    band_low = (band - band_high.astype(jnp.float32)).astype(jnp.bfloat16)
    weights[...] = jnp.concatenate(
        [
            jnp.concatenate([band_high, band_low], axis=1),
            jnp.concatenate([band_high, jnp.zeros_like(band_low)], axis=1),
        ],
        axis=0,
    )

    def along(v):
        tall = v.reshape(GROUP * width, length)
        high = tall.astype(jnp.bfloat16)
        low = (tall - high.astype(jnp.float32)).astype(jnp.bfloat16)
        both = jnp.dot(
            jnp.concatenate([high, low], axis=1), weights[...], preferred_element_type=jnp.float32
        )
        return (both[:, :length] + both[:, length:]).reshape(GROUP, width, length)

    local[6].wait()
    origin = sdepth_v[...]

    def advance(t, z, old):
        own = pl.ds(REACH, width)
        v = field[t, pl.ds(REACH + z, GROUP), own, :]
        total = (3.0 * CENTER) * v if ny > 1 else along(v)
        for k in range(1, REACH + 1):
            near = (
                field[t, pl.ds(REACH + z + k, GROUP), own, :]
                + field[t, pl.ds(REACH + z - k, GROUP), own, :]
            )
            near = near + (
                field[t, pl.ds(REACH + z, GROUP), pl.ds(REACH + k, width), :]
                + field[t, pl.ds(REACH + z, GROUP), pl.ds(REACH - k, width), :]
            )
            total = total + COEFS[k - 1] * near
            if ny > 1:
                up = pltpu.roll(v, length - k, 2)
                down = pltpu.roll(v, k, 2)
                low = pltpu.roll(side[t, 0, pl.ds(z, GROUP), :, :], k, 2)
                high = pltpu.roll(side[t, 1, pl.ds(z, GROUP), :, :], length - k, 2)
                up = jnp.where((lanes < length - k)[None], up, high)
                down = jnp.where((lanes >= k)[None], down, low)
                total = total + COEFS[k - 1] * (up + down)
        strength = courant_v[pl.ds(z, GROUP), :, :].astype(jnp.float32)
        levels = lax.broadcasted_iota(jnp.int32, (GROUP, width, length), 0) + z
        shot = jnp.where(levels == origin[None], amp[t][None], 0.0)
        return 2.0 * v - old + strength * total + shot

    def first_chunk(c, carry):
        arrived(0, c)

        def group(g, inner):
            z = c * rows + g * GROUP
            new = advance(0, z, prior_v[pl.ds(z, GROUP), :, :])
            field[1, pl.ds(REACH + z, GROUP), pl.ds(REACH, width), :] = new
            return inner

        lax.fori_loop(0, rows // GROUP, group, 0, unroll=True)
        send(1, c)
        return carry

    lax.fori_loop(0, CHUNKS, first_chunk, 0)

    def step(i, carry):
        t = i // CHUNKS
        c = i % CHUNKS
        arrived(t, c)

        def group(g, inner):
            z = c * rows + g * GROUP
            old = field[t - 1, pl.ds(REACH + z, GROUP), pl.ds(REACH, width), :]
            new = advance(t, z, old)
            field[t + 1, pl.ds(REACH + z, GROUP), pl.ds(REACH, width), :] = new
            return inner

        lax.fori_loop(0, rows // GROUP, group, 0, unroll=True)

        @pl.when(t < STEPS - 1)
        def _():
            send(t + 1, c)

        return carry

    lax.fori_loop(CHUNKS, STEPS * CHUNKS, step, 0)

    done = pltpu.make_async_copy(
        field.at[STEPS, pl.ds(REACH, depth), pl.ds(REACH, width), :], final, out_sem.at[0]
    )
    done.start()

    local[3].wait()
    local[7].wait()
    ground = rdepth_v[...]
    product[pl.ds(0, 1), :, :] = jnp.zeros((1, width, length), jnp.float32)
    product[pl.ds(depth + 1, 1), :, :] = jnp.zeros((1, width, length), jnp.float32)

    def multiply(g, carry):
        z = g * GROUP
        levels = lax.broadcasted_iota(jnp.int32, (GROUP, width, length), 0) + z
        masked = jnp.where(levels >= ground[None], receiver_v[pl.ds(z, GROUP), :, :], 0.0)
        product[pl.ds(1 + z, GROUP), :, :] = (
            field[STEPS, pl.ds(REACH + z, GROUP), pl.ds(REACH, width), :] * masked
        )
        return carry

    lax.fori_loop(0, depth // GROUP, multiply, 0)

    def landing(who):
        return image.at[:, pl.ds(pl.multiple_of(who * width, width), width), :]

    def piece(peer):
        return pltpu.make_async_remote_copy(
            src_ref=slab.at[pl.ds(peer * slab_depth, slab_depth), :, :],
            dst_ref=landing(me),
            send_sem=img_send.at[peer],
            recv_sem=img_recv.at[me],
            device_id={"gx": peer},
            device_id_type=pl.DeviceIdType.MESH,
        )

    def kept():
        return pltpu.make_async_copy(
            slab.at[pl.ds(me * slab_depth, slab_depth), :, :], landing(me), out_sem.at[1]
        )

    def filtered(peer):
        z = peer * slab_depth
        slab[pl.ds(z, slab_depth), :, :] = (
            2.0 * product[pl.ds(1 + z, slab_depth), :, :]
            - product[pl.ds(z, slab_depth), :, :]
            - product[pl.ds(2 + z, slab_depth), :, :]
        )

    def ship(j, carry):
        peer = lax.rem(me + j, nx)
        filtered(peer)
        piece(peer).start()
        return carry

    lax.fori_loop(1, nx, ship, 0)
    filtered(me)
    kept().start()

    def drain(i, carry):
        sent(i // CHUNKS, i % CHUNKS)
        return carry

    lax.fori_loop(0, STEPS * CHUNKS, drain, 0)

    def finish(j, carry):
        peer = lax.rem(me + j, nx)
        piece(peer).wait_send()
        came = lax.rem(me + nx - j, nx)
        pltpu.make_async_remote_copy(
            src_ref=slab.at[pl.ds(me * slab_depth, slab_depth), :, :],
            dst_ref=landing(came),
            send_sem=img_send.at[came],
            recv_sem=img_recv.at[came],
            device_id={"gx": came},
            device_id_type=pl.DeviceIdType.MESH,
        ).wait_recv()
        return carry

    lax.fori_loop(1, nx, finish, 0)
    kept().wait()
    done.wait()


def solution(mesh):
    nx, ny = mesh.shape["gx"], mesh.shape["gy"]

    def shards(
        pressure, prior, courant, wavelet, delay, sdepth, rdepth, receiver
    ):
        depth, width, length = pressure.shape
        hbm = pl.BlockSpec(memory_space=pl.ANY)
        flat = (depth, width, length)
        sides = (STEPS, 2, depth, width, length) if ny > 1 else (1, 1, 1, width, length)
        return pl.pallas_call(
            functools.partial(kernel, nx, ny),
            out_shape=(
                jax.ShapeDtypeStruct(flat, jnp.float32),
                jax.ShapeDtypeStruct((depth // nx, width * nx, length), jnp.float32),
            ),
            in_specs=[hbm] * 8,
            out_specs=(hbm, hbm),
            scratch_shapes=[
                pltpu.VMEM((STEPS + 1, depth + 2 * REACH, width + 2 * REACH, length), jnp.float32),
                pltpu.VMEM(sides, jnp.float32),
                pltpu.VMEM(flat, jnp.float32),
                pltpu.VMEM(flat, jnp.bfloat16),
                pltpu.VMEM(flat, jnp.float32),
                pltpu.VMEM((STEPS, width, length), jnp.float32),
                pltpu.VMEM((depth + 2, width, length), jnp.float32),
                pltpu.VMEM(flat, jnp.float32),
                pltpu.VMEM((2 * length, 2 * length), jnp.bfloat16),
                pltpu.SMEM(wavelet.shape, jnp.float32),
                pltpu.VMEM((width, length), jnp.int32),
                pltpu.VMEM((width, length), jnp.int32),
                pltpu.VMEM((width, length), jnp.int32),
                pltpu.SemaphoreType.DMA((8,)),
                pltpu.SemaphoreType.DMA((STEPS, CHUNKS, 2)),
                pltpu.SemaphoreType.DMA((STEPS, CHUNKS, 2)),
                pltpu.SemaphoreType.DMA((STEPS, CHUNKS, 2)),
                pltpu.SemaphoreType.DMA((STEPS, CHUNKS, 2)),
                pltpu.SemaphoreType.DMA((2,)),
                pltpu.SemaphoreType.DMA((nx,)),
                pltpu.SemaphoreType.DMA((nx,)),
            ],
            compiler_params=pltpu.CompilerParams(
                collective_id=0, has_side_effects=True, vmem_limit_bytes=67043328
            ),
        )(pressure, prior, courant, wavelet, delay, sdepth, rdepth, receiver)

    in_specs = (
        P(None, ("shots", "gx"), "gy"),
        P(None, ("shots", "gx"), "gy"),
        P(None, "gx", "gy"),
        P("shots"),
        P(("shots", "gx"), "gy"),
        P(("shots", "gx"), "gy"),
        P(("shots", "gx"), "gy"),
        P(None, ("shots", "gx"), "gy"),
    )
    out_specs = (P(None, ("shots", "gx"), "gy"), P("gx", "shots", "gy"))
    return jax.shard_map(shards, mesh=mesh, in_specs=in_specs, out_specs=out_specs, check_vma=False)
```

```python
import functools

import jax
import jax.numpy as jnp
from jax import lax
from jax.experimental import pallas as pl
from jax.experimental.pallas import tpu as pltpu
from jax.sharding import PartitionSpec as P

STEPS = 8
REACH = 4
CENTER = -205.0 / 72.0
COEFS = (1.6, -0.2, 8.0 / 315.0, -1.0 / 560.0)
CHUNKS = 2
GROUP = 8


def kernel(
    nx,
    ny,
    pressure,
    prior,
    courant,
    wavelet,
    delay,
    sdepth,
    rdepth,
    receiver,
    final,
    image,
    field,
    side,
    prior_v,
    courant_v,
    receiver_v,
    amp,
    product,
    slab,
    weights,
    wave_v,
    delay_v,
    sdepth_v,
    rdepth_v,
    local_sem,
    send_sem,
    recv_sem,
    side_send,
    side_recv,
    out_sem,
    img_send,
    img_recv,
    known,
):
    depth, width, length = pressure.shape
    rows = depth // CHUNKS
    slab_depth = depth // nx
    me = lax.axis_index("gx")
    mine = lax.axis_index("gy")

    local = [
        pltpu.make_async_copy(
            pressure, field.at[0, pl.ds(REACH, depth), pl.ds(REACH, width), :], local_sem.at[0]
        ),
        pltpu.make_async_copy(prior, prior_v, local_sem.at[1]),
        pltpu.make_async_copy(courant, courant_v, local_sem.at[2]),
        pltpu.make_async_copy(receiver, receiver_v, local_sem.at[3]),
        pltpu.make_async_copy(wavelet, wave_v, local_sem.at[4]),
        pltpu.make_async_copy(delay, delay_v, local_sem.at[5]),
        pltpu.make_async_copy(sdepth, sdepth_v, local_sem.at[6]),
        pltpu.make_async_copy(rdepth, rdepth_v, local_sem.at[7]),
    ]
    for copy in local:
        copy.start()

    barrier = pltpu.get_barrier_semaphore()
    beside = sorted({1, nx - 1} - {0}) if nx > 1 else []
    for j in beside:
        pl.semaphore_signal(
            barrier,
            inc=1,
            device_id={"gx": lax.rem(me + j, nx)},
            device_id_type=pl.DeviceIdType.MESH,
        )
    for j in range(1, ny):
        pl.semaphore_signal(
            barrier,
            inc=1,
            device_id={"gy": lax.rem(mine + j, ny)},
            device_id_type=pl.DeviceIdType.MESH,
        )

    rim = jnp.zeros((REACH, width + 2 * REACH, length), jnp.float32)
    for t in range(STEPS):
        field[t, pl.ds(0, REACH), :, :] = rim
        field[t, pl.ds(REACH + depth, REACH), :, :] = rim

    def clear(at):
        def one(i, carry):
            t = i // CHUNKS
            c = i % CHUNKS
            field[t, pl.ds(REACH + c * rows, rows), pl.ds(at, REACH), :] = jnp.zeros(
                (rows, REACH, length), jnp.float32
            )
            return carry

        lax.fori_loop(0, STEPS * CHUNKS, one, 0)

    @pl.when(me == 0)
    def _():
        clear(0)

    @pl.when(me == nx - 1)
    def _():
        clear(REACH + width)

    if ny > 1:

        def clear_side(k):
            def one(i, carry):
                t = i // CHUNKS
                c = i % CHUNKS
                side[t, k, pl.ds(c * rows, rows), :, :] = jnp.zeros(
                    (rows, width, length), jnp.float32
                )
                return carry

            lax.fori_loop(0, STEPS * CHUNKS, one, 0)

        @pl.when(mine == 0)
        def _():
            clear_side(0)

        @pl.when(mine == ny - 1)
        def _():
            clear_side(1)

    local[4].wait()
    local[5].wait()
    late = delay_v[...]
    for t in range(STEPS):
        total = jnp.zeros((width, length), jnp.float32)
        for pick in range(wavelet.shape[0]):
            total = total + jnp.where(late + t == pick, wave_v[pick], 0.0)
        amp[t] = total

    if len(beside) + ny > 1:
        pl.semaphore_wait(barrier, len(beside) + ny - 1)

    def span(c):
        return pl.ds(REACH + c * rows, rows)

    def face(t, c, way):
        source = REACH + width - REACH if way == 0 else REACH
        target = 0 if way == 0 else REACH + width
        peer = lax.rem(me + 1, nx) if way == 0 else lax.rem(me + nx - 1, nx)
        return pltpu.make_async_remote_copy(
            src_ref=field.at[t, span(c), pl.ds(source, REACH), :],
            dst_ref=field.at[t, span(c), pl.ds(target, REACH), :],
            send_sem=send_sem.at[t, c, way],
            recv_sem=recv_sem.at[t, c, way],
            device_id={"gx": peer},
            device_id_type=pl.DeviceIdType.MESH,
        )

    def flank(t, c, way):
        peer = lax.rem(mine + 1, ny) if way == 0 else lax.rem(mine + ny - 1, ny)
        return pltpu.make_async_remote_copy(
            src_ref=field.at[t, span(c), pl.ds(REACH, width), :],
            dst_ref=side.at[t, way, pl.ds(c * rows, rows), :, :],
            send_sem=side_send.at[t, c, way],
            recv_sem=side_recv.at[t, c, way],
            device_id={"gy": peer},
            device_id_type=pl.DeviceIdType.MESH,
        )

    def each_face(t, c, act, sending):
        lower, upper = (me > 0, me < nx - 1)
        if nx > 1:
            for way in (0, 1):
                there = upper if (way == 0) == sending else lower

                @pl.when(there)
                def _():
                    act(face(t, c, way))

        if ny > 1:
            for way in (0, 1):
                there = mine < ny - 1 if (way == 0) == sending else mine > 0

                @pl.when(there)
                def _():
                    act(flank(t, c, way))

    def send(t, c):
        each_face(t, c, lambda copy: copy.start(), True)

    def sent(t, c):
        each_face(t, c, lambda copy: copy.wait_send(), True)

    def arrived(t, c):
        each_face(t, c, lambda copy: copy.wait_recv(), False)

    local[0].wait()
    for c in range(CHUNKS):
        send(0, c)
    local[1].wait()
    local[2].wait()

    lanes = lax.broadcasted_iota(jnp.int32, (width, length), 1)
    start = lax.broadcasted_iota(jnp.int32, (length, length), 0)
    gap = jnp.abs(start - lax.broadcasted_iota(jnp.int32, (length, length), 1))
    band = jnp.where(gap == 0, 3.0 * CENTER, 0.0)
    for k in range(1, REACH + 1):
        band = jnp.where(gap == k, COEFS[k - 1], band)
    band_high = band.astype(jnp.bfloat16)
    band_low = (band - band_high.astype(jnp.float32)).astype(jnp.bfloat16)
    weights[...] = jnp.concatenate(
        [
            jnp.concatenate([band_high, band_low], axis=1),
            jnp.concatenate([band_high, jnp.zeros_like(band_low)], axis=1),
        ],
        axis=0,
    )

    def along(v):
        tall = v.reshape(GROUP * width, length)
        high = tall.astype(jnp.bfloat16)
        low = (tall - high.astype(jnp.float32)).astype(jnp.bfloat16)
        both = jnp.dot(
            jnp.concatenate([high, low], axis=1), weights[...], preferred_element_type=jnp.float32
        )
        return (both[:, :length] + both[:, length:]).reshape(GROUP, width, length)

    local[6].wait()
    origin = sdepth_v[...]

    def advance(t, z, old):
        own = pl.ds(REACH, width)
        v = field[t, pl.ds(REACH + z, GROUP), own, :]
        total = (3.0 * CENTER) * v if ny > 1 else along(v)
        for k in range(1, REACH + 1):
            near = (
                field[t, pl.ds(REACH + z + k, GROUP), own, :]
                + field[t, pl.ds(REACH + z - k, GROUP), own, :]
            )
            near = near + (
                field[t, pl.ds(REACH + z, GROUP), pl.ds(REACH + k, width), :]
                + field[t, pl.ds(REACH + z, GROUP), pl.ds(REACH - k, width), :]
            )
            total = total + COEFS[k - 1] * near
            if ny > 1:
                up = pltpu.roll(v, length - k, 2)
                down = pltpu.roll(v, k, 2)
                low = pltpu.roll(side[t, 0, pl.ds(z, GROUP), :, :], k, 2)
                high = pltpu.roll(side[t, 1, pl.ds(z, GROUP), :, :], length - k, 2)
                up = jnp.where((lanes < length - k)[None], up, high)
                down = jnp.where((lanes >= k)[None], down, low)
                total = total + COEFS[k - 1] * (up + down)
        strength = courant_v[pl.ds(z, GROUP), :, :].astype(jnp.float32)
        levels = lax.broadcasted_iota(jnp.int32, (GROUP, width, length), 0) + z
        shot = jnp.where(levels == origin[None], amp[t][None], 0.0)
        return 2.0 * v - old + strength * total + shot

    def first_chunk(c, carry):
        arrived(0, c)

        def group(g, inner):
            z = c * rows + g * GROUP
            new = advance(0, z, prior_v[pl.ds(z, GROUP), :, :])
            field[1, pl.ds(REACH + z, GROUP), pl.ds(REACH, width), :] = new
            return inner

        lax.fori_loop(0, rows // GROUP, group, 0, unroll=True)
        send(1, c)
        return carry

    lax.fori_loop(0, CHUNKS, first_chunk, 0)

    reach = []
    while (reach[-1] * 2 if reach else 1) < nx // 2:
        reach.append(reach[-1] * 2 if reach else 1)

    def greet(number):
        for way, j in enumerate((reach[number], nx - reach[number])):
            pl.semaphore_signal(
                known.at[number, way],
                inc=1,
                device_id={"gx": lax.rem(me + j, nx)},
                device_id_type=pl.DeviceIdType.MESH,
            )

    def greeted(number):
        for way in (0, 1):
            pl.semaphore_wait(known.at[number, way], 1)

    def meet(number):
        if number > 0:
            greeted(number - 1)
        greet(number)

    def step(i, carry):
        t = i // CHUNKS
        c = i % CHUNKS
        for number in range(len(reach)):
            if CHUNKS + 3 * number < STEPS * CHUNKS:

                @pl.when(i == CHUNKS + 3 * number)
                def _():
                    meet(number)

        arrived(t, c)

        def group(g, inner):
            z = c * rows + g * GROUP
            old = field[t - 1, pl.ds(REACH + z, GROUP), pl.ds(REACH, width), :]
            new = advance(t, z, old)
            field[t + 1, pl.ds(REACH + z, GROUP), pl.ds(REACH, width), :] = new
            return inner

        lax.fori_loop(0, rows // GROUP, group, 0, unroll=True)

        @pl.when(t < STEPS - 1)
        def _():
            send(t + 1, c)

        return carry

    lax.fori_loop(CHUNKS, STEPS * CHUNKS, step, 0)
    for number in range(len(reach)):
        if CHUNKS + 3 * number >= STEPS * CHUNKS:
            meet(number)
    if reach:
        greeted(len(reach) - 1)

    done = pltpu.make_async_copy(
        field.at[STEPS, pl.ds(REACH, depth), pl.ds(REACH, width), :], final, out_sem.at[0]
    )
    done.start()

    local[3].wait()
    local[7].wait()
    ground = rdepth_v[...]
    product[pl.ds(0, 1), :, :] = jnp.zeros((1, width, length), jnp.float32)
    product[pl.ds(depth + 1, 1), :, :] = jnp.zeros((1, width, length), jnp.float32)

    def multiply(g, carry):
        z = g * GROUP
        levels = lax.broadcasted_iota(jnp.int32, (GROUP, width, length), 0) + z
        masked = jnp.where(levels >= ground[None], receiver_v[pl.ds(z, GROUP), :, :], 0.0)
        product[pl.ds(1 + z, GROUP), :, :] = (
            field[STEPS, pl.ds(REACH + z, GROUP), pl.ds(REACH, width), :] * masked
        )
        return carry

    lax.fori_loop(0, depth // GROUP, multiply, 0)

    def landing(who):
        return image.at[:, pl.ds(pl.multiple_of(who * width, width), width), :]

    def piece(peer):
        return pltpu.make_async_remote_copy(
            src_ref=slab.at[pl.ds(peer * slab_depth, slab_depth), :, :],
            dst_ref=landing(me),
            send_sem=img_send.at[peer],
            recv_sem=img_recv.at[me],
            device_id={"gx": peer},
            device_id_type=pl.DeviceIdType.MESH,
        )

    def kept():
        return pltpu.make_async_copy(
            slab.at[pl.ds(me * slab_depth, slab_depth), :, :], landing(me), out_sem.at[1]
        )

    def filtered(peer):
        z = peer * slab_depth
        slab[pl.ds(z, slab_depth), :, :] = (
            2.0 * product[pl.ds(1 + z, slab_depth), :, :]
            - product[pl.ds(z, slab_depth), :, :]
            - product[pl.ds(2 + z, slab_depth), :, :]
        )

    def ship(j, carry):
        peer = lax.rem(me + j, nx)
        filtered(peer)
        piece(peer).start()
        return carry

    lax.fori_loop(1, nx, ship, 0)
    filtered(me)
    kept().start()

    def drain(i, carry):
        sent(i // CHUNKS, i % CHUNKS)
        return carry

    lax.fori_loop(0, STEPS * CHUNKS, drain, 0)

    def finish(j, carry):
        peer = lax.rem(me + j, nx)
        piece(peer).wait_send()
        came = lax.rem(me + nx - j, nx)
        pltpu.make_async_remote_copy(
            src_ref=slab.at[pl.ds(me * slab_depth, slab_depth), :, :],
            dst_ref=landing(came),
            send_sem=img_send.at[came],
            recv_sem=img_recv.at[came],
            device_id={"gx": came},
            device_id_type=pl.DeviceIdType.MESH,
        ).wait_recv()
        return carry

    lax.fori_loop(1, nx, finish, 0)
    kept().wait()
    done.wait()


def solution(mesh):
    nx, ny = mesh.shape["gx"], mesh.shape["gy"]

    def shards(
        pressure, prior, courant, wavelet, delay, sdepth, rdepth, receiver
    ):
        depth, width, length = pressure.shape
        hbm = pl.BlockSpec(memory_space=pl.ANY)
        flat = (depth, width, length)
        sides = (STEPS, 2, depth, width, length) if ny > 1 else (1, 1, 1, width, length)
        return pl.pallas_call(
            functools.partial(kernel, nx, ny),
            out_shape=(
                jax.ShapeDtypeStruct(flat, jnp.float32),
                jax.ShapeDtypeStruct((depth // nx, width * nx, length), jnp.float32),
            ),
            in_specs=[hbm] * 8,
            out_specs=(hbm, hbm),
            scratch_shapes=[
                pltpu.VMEM((STEPS + 1, depth + 2 * REACH, width + 2 * REACH, length), jnp.float32),
                pltpu.VMEM(sides, jnp.float32),
                pltpu.VMEM(flat, jnp.float32),
                pltpu.VMEM(flat, jnp.bfloat16),
                pltpu.VMEM(flat, jnp.float32),
                pltpu.VMEM((STEPS, width, length), jnp.float32),
                pltpu.VMEM((depth + 2, width, length), jnp.float32),
                pltpu.VMEM(flat, jnp.float32),
                pltpu.VMEM((2 * length, 2 * length), jnp.bfloat16),
                pltpu.SMEM(wavelet.shape, jnp.float32),
                pltpu.VMEM((width, length), jnp.int32),
                pltpu.VMEM((width, length), jnp.int32),
                pltpu.VMEM((width, length), jnp.int32),
                pltpu.SemaphoreType.DMA((8,)),
                pltpu.SemaphoreType.DMA((STEPS, CHUNKS, 2)),
                pltpu.SemaphoreType.DMA((STEPS, CHUNKS, 2)),
                pltpu.SemaphoreType.DMA((STEPS, CHUNKS, 2)),
                pltpu.SemaphoreType.DMA((STEPS, CHUNKS, 2)),
                pltpu.SemaphoreType.DMA((2,)),
                pltpu.SemaphoreType.DMA((nx,)),
                pltpu.SemaphoreType.DMA((nx,)),
                pltpu.SemaphoreType.REGULAR((max(nx.bit_length(), 1), 2)),
            ],
            compiler_params=pltpu.CompilerParams(
                collective_id=0, has_side_effects=True, vmem_limit_bytes=67043328
            ),
        )(pressure, prior, courant, wavelet, delay, sdepth, rdepth, receiver)

    in_specs = (
        P(None, ("shots", "gx"), "gy"),
        P(None, ("shots", "gx"), "gy"),
        P(None, "gx", "gy"),
        P("shots"),
        P(("shots", "gx"), "gy"),
        P(("shots", "gx"), "gy"),
        P(("shots", "gx"), "gy"),
        P(None, ("shots", "gx"), "gy"),
    )
    out_specs = (P(None, ("shots", "gx"), "gy"), P("gx", "shots", "gy"))
    return jax.shard_map(shards, mesh=mesh, in_specs=in_specs, out_specs=out_specs, check_vma=False)
```
